32 devices in a mesh: wide: 8 (over z, y), narrow: 4 (over x, core).
Axes of the slice: x: 2, y: 2, z: 4, core: 2. Of those that a mesh axis runs over, the one named last changes fastest.
Arguments:
- tokens: bfloat16 [32768, 768], P(('wide', 'narrow')), may hold values from -6 to 6
- lengths: int32 [32], P(('wide', 'narrow')), may hold values from 512 to 1024, as said below
- query_weight: bfloat16 [768, 768], P(('wide', 'narrow')), may hold values from -0.25 to 0.25
- key_weight: bfloat16 [768, 768], P(('wide', 'narrow')), may hold values from -0.25 to 0.25
- value_weight: bfloat16 [768, 768], P(('wide', 'narrow')), may hold values from -0.21875 to 0.21875
- query_bias: bfloat16 [768], P(('wide', 'narrow')), may hold values from -3 to 3
- value_bias: bfloat16 [768], P(('wide', 'narrow')), may hold values from -3 to 3
- conv_weight: bfloat16 [12, 33], replicated, may hold values from -0.29882812 to 0.29882812
- output_weight: bfloat16 [768, 768], P(('wide', 'narrow')), may hold values from -0.875 to 0.875
- output_bias: bfloat16 [768], P(('wide', 'narrow')), may hold values from -3 to 3
- norm_gain: bfloat16 [768], P(('wide', 'narrow')), may hold values from 0.5 to 1.5
- norm_bias: bfloat16 [768], P(('wide', 'narrow')), may hold values from -1.796875 to 1.796875
- up_weight: bfloat16 [768, 3072], P(('wide', 'narrow')), may hold values from -0.21875 to 0.21875
- up_bias: bfloat16 [3072], P(('wide', 'narrow')), may hold values from -3 to 3
- down_weight: bfloat16 [3072, 768], P(('wide', 'narrow')), may hold values from -0.109375 to 0.109375
- down_bias: bfloat16 [768], P(('wide', 'narrow')), may hold values from -1.796875 to 1.796875
- final_gain: bfloat16 [768], P(('wide', 'narrow')), may hold values from 0.5 to 1.5
- final_bias: bfloat16 [768], P(('wide', 'narrow')), may hold values from -1.796875 to 1.796875
- cotangent: bfloat16 [32768, 768], P(('wide', 'narrow')), may hold values from -6 to 6
Outputs:
- result: float32 [32768, 768], P(('wide', 'narrow'))
- tokens_grad: float32 [32768, 768], P(('wide', 'narrow'))
- query_weight_grad: float32 [768, 768], P(('wide', 'narrow'))
- key_weight_grad: float32 [768, 768], P(('wide', 'narrow'))
- value_weight_grad: float32 [768, 768], P(('wide', 'narrow'))
- query_bias_grad: float32 [768], P(('wide', 'narrow'))
- value_bias_grad: float32 [768], P(('wide', 'narrow'))
- conv_weight_grad: float32 [12, 33], replicated
- output_weight_grad: float32 [768, 768], P(('wide', 'narrow'))
- output_bias_grad: float32 [768], P(('wide', 'narrow'))
- norm_gain_grad: float32 [768], P(('wide', 'narrow'))
- norm_bias_grad: float32 [768], P(('wide', 'narrow'))
- up_weight_grad: float32 [768, 3072], P(('wide', 'narrow'))
- up_bias_grad: float32 [3072], P(('wide', 'narrow'))
- down_weight_grad: float32 [3072, 768], P(('wide', 'narrow'))
- down_bias_grad: float32 [768], P(('wide', 'narrow'))
- final_gain_grad: float32 [768], P(('wide', 'narrow'))
- final_bias_grad: float32 [768], P(('wide', 'narrow'))
- proxy: float32 [12], replicated
The draws below stay inside these ranges and needn't reach their ends.
Inputs may be any that keep to these rules, and one draw needn't show every extreme that they name: `lengths`: each sequence's true length; its positions from that length on are padding.
All inputs are finite; a program needn't handle non-finite values.
Results may differ from the reference program's by a relative error of at most 0.009.
Values may be sent and summed in bfloat16 or wider, within the bound.
A program may use at most 320 MiB of HBM per device.

```python
import jax
import jax.numpy as jnp
from jax import lax

D = 768
HEADS = 12
FF = 3072
MARKS = 64
CONV_WIDTH = 33
NEWTON = 6
LEN = 1024
SEQS = 32
TOKENS = 32768


def draw_lengths(key, part):
    first, second = jax.random.split(key, 2)
    values = jax.random.randint(first, (SEQS,), LEN // 2, LEN + 1)
    order = jax.random.permutation(second, SEQS)
    values = jnp.where(order == 0, LEN, values)
    values = jnp.where(order == 1, LEN // 2, values)
    return values.astype(jnp.int32)


def level_of(key, shape, shards, least, high):
    level, own = 1.0, jax.random.fold_in(key, 6)
    for dim, shards_of in shards:
        heights = jnp.exp(jax.random.uniform(jax.random.fold_in(own, dim), (shards_of,), jnp.float32, least / len(shards), high / len(shards)))
        level = level * jnp.repeat(heights, shape[dim] // shards_of).reshape([-1 if axis == dim else 1 for axis in range(len(shape))])
    return level


def gaussian(rng, shape, scale, limit, cuts=(), held_as=jnp.bfloat16):
    entries = scale * jax.random.normal(rng, shape, jnp.float32)
    if cuts:
        entries = entries * level_of(rng, shape, cuts, -0.22, 0.18)
    return jnp.clip(entries, -limit, limit).astype(held_as)


def setup_inputs(seed: int = 0) -> dict:
    seeds = jax.random.split(jax.random.key(seed), 20)
    return {
        "tokens": gaussian(seeds[0], (TOKENS, D), 1.0, 6.0, ((0, 32),)),
        "lengths": draw_lengths(jax.random.fold_in(seeds[19], 71), 0),
        "query_weight": gaussian(seeds[2], (D, D), (D * 2 // 3) ** -0.5, 0.25, ((0, 32),)),
        "key_weight": gaussian(seeds[3], (D, D), (D * 2 // 3) ** -0.5, 0.25, ((0, 32),)),
        "value_weight": gaussian(seeds[4], (D, D), D ** -0.5, 0.21875, ((0, 32),)),
        "query_bias": gaussian(seeds[5], (D,), 0.5, 3.0, ((0, 32),)),
        "value_bias": gaussian(seeds[6], (D,), 0.5, 3.0, ((0, 32),)),
        "conv_weight": gaussian(seeds[7], (HEADS, CONV_WIDTH), 0.05, 0.29882812),
        "output_weight": gaussian(seeds[8], (D, D), (D // 16) ** -0.5, 0.875, ((0, 32),)),
        "output_bias": gaussian(seeds[9], (D,), 0.5, 3.0, ((0, 32),)),
        "norm_gain": jnp.clip(1.0 + 0.1 * jax.random.normal(seeds[10], (D,), jnp.float32), 0.5, 1.5).astype(jnp.bfloat16),
        "norm_bias": gaussian(seeds[11], (D,), 0.3, 1.796875, ((0, 32),)),
        "up_weight": gaussian(seeds[12], (D, FF), D ** -0.5, 0.21875, ((0, 32),)),
        "up_bias": gaussian(seeds[13], (FF,), 0.5, 3.0, ((0, 32),)),
        "down_weight": gaussian(seeds[14], (FF, D), FF ** -0.5, 0.109375, ((0, 32),)),
        "down_bias": gaussian(seeds[15], (D,), 0.3, 1.796875, ((0, 32),)),
        "final_gain": jnp.clip(1.0 + 0.1 * jax.random.normal(seeds[16], (D,), jnp.float32), 0.5, 1.5).astype(jnp.bfloat16),
        "final_bias": gaussian(seeds[17], (D,), 0.3, 1.796875, ((0, 32),)),
        "cotangent": gaussian(seeds[18], (TOKENS, D), 1.0, 6.0, ((0, 32),)),
    }


EPSILON = 1e-05
MASKED_SCORE = 1000000000.0

@jax.custom_vjp
def low(v):
    return lax.optimization_barrier(v.astype(jnp.bfloat16)).astype(jnp.float32)

@jax.custom_vjp
def low_back(v):
    return v

def low_keep(v):
    return (low(v), None)

def low_pass(kept, grad):
    return (grad,)

def back_keep(v):
    return (v, None)

def back_low(kept, grad):
    return (low(grad),)
low.defvjp(low_keep, low_pass)
low_back.defvjp(back_keep, back_low)

def batch_mapped(form, left, right):
    return jnp.einsum(form, left, right, precision=lax.Precision.HIGHEST, preferred_element_type=jnp.float32)

def matmul_high(left, right):
    return jnp.dot(left, right, precision=lax.Precision.HIGHEST, preferred_element_type=jnp.float32)

def softmax_final_axis(scores):
    top = lax.optimization_barrier(jnp.max(scores, axis=-1, keepdims=True))
    powers = jnp.exp(scores - top)
    return powers / lax.optimization_barrier(jnp.sum(powers, axis=-1, keepdims=True))

def newton_inverse(kernel):
    marks = kernel.shape[-1]
    identity = jnp.eye(marks, dtype=jnp.float32)
    column_max = lax.optimization_barrier(jnp.max(lax.optimization_barrier(jnp.sum(kernel, axis=-2)), axis=-1))
    pseudo_inverse = jnp.swapaxes(kernel, -1, -2) / column_max[:, None, None]
    for sweep in range(NEWTON):
        product = batch_mapped('hmn,hnp->hmp', kernel, pseudo_inverse)
        inner = 7.0 * identity - product
        inner = 15.0 * identity - batch_mapped('hmn,hnp->hmp', product, inner)
        inner = 13.0 * identity - batch_mapped('hmn,hnp->hmp', product, inner)
        pseudo_inverse = 0.25 * batch_mapped('hmn,hnp->hmp', pseudo_inverse, inner)
    return pseudo_inverse

def attention_core(queries, keys, values, conv_weight, length):
    seq_len = queries.shape[0]
    heads = conv_weight.shape[0]
    width = conv_weight.shape[1]
    head_dim = queries.shape[1] // heads
    scale = head_dim ** (-0.25)
    marks = MARKS
    position = jnp.arange(seq_len, dtype=jnp.int32)
    valid_mask = (position < length).astype(jnp.float32)
    marker = jnp.arange(marks, dtype=jnp.int32)
    lower = marker * length // marks
    upper = (marker + 1) * length // marks
    inside = jnp.logical_and(position[None, :] >= lower[:, None], position[None, :] < upper[:, None])
    counts = (upper - lower).astype(jnp.float32)
    segment_averager = inside.astype(jnp.float32) / counts[:, None]
    query_per_head = (queries * scale).reshape(seq_len, heads, head_dim)
    key_per_head = (keys * scale).reshape(seq_len, heads, head_dim)
    value_per_head = (values * valid_mask[:, None]).reshape(seq_len, heads, head_dim)
    query_landmarks = batch_mapped('vi,iqj->qvj', segment_averager, query_per_head)
    key_landmarks = batch_mapped('vi,iqj->qvj', segment_averager, key_per_head)
    first_kernel = softmax_final_axis(batch_mapped('bsz,scz->sbc', query_per_head, key_landmarks))
    second_kernel = softmax_final_axis(batch_mapped('pus,pos->puo', query_landmarks, key_landmarks))
    third_score_matrix = batch_mapped('ncf,xnf->ncx', query_landmarks, key_per_head) + (valid_mask - 1.0) * MASKED_SCORE
    third_kernel = softmax_final_axis(third_score_matrix)
    landmark_value_rows = batch_mapped('iob,bia->ioa', third_kernel, value_per_head)
    pseudo_inverse = newton_inverse(second_kernel)
    mixed_output = batch_mapped('xkc,xcl->xkl', pseudo_inverse, landmark_value_rows)
    nystrom_attention = batch_mapped('bqj,bjg->qbg', first_kernel, mixed_output)
    half = (width - 1) // 2
    padded = jnp.pad(value_per_head, ((half, half), (0, 0), (0, 0)))
    convolved = jnp.zeros_like(value_per_head)
    for offset in range(width):
        convolved = convolved + conv_weight[:, offset][None, :, None] * padded[offset:offset + seq_len]
    context = ((nystrom_attention + convolved) * valid_mask[:, None, None]).reshape(seq_len, heads * head_dim)
    proxy = jnp.sqrt(lax.optimization_barrier(jnp.sum(second_kernel * second_kernel, axis=(1, 2)))) * jnp.sqrt(lax.optimization_barrier(jnp.sum(pseudo_inverse * pseudo_inverse, axis=(1, 2)))) / marks
    return (context, proxy)

def layer_norm(rows, gain, shift):
    centered = rows - lax.optimization_barrier(jnp.mean(rows, axis=-1, keepdims=True))
    variance = lax.optimization_barrier(jnp.mean(centered * centered, axis=-1, keepdims=True))
    return centered * lax.rsqrt(variance + EPSILON) * gain + shift

def gelu_exact(values):
    return 0.5 * values * (1.0 + jax.scipy.special.erf(values * 0.5 ** 0.5))

def forward(rows, params, length):
    query_weight, key_weight, value_weight, query_bias, value_bias, conv_weight, output_weight, output_bias, norm_gain, norm_bias, up_weight, up_bias, down_weight, down_bias, final_gain, final_bias = params
    queries = low_back(matmul_high(rows, query_weight) + query_bias)
    keys = low_back(matmul_high(rows, key_weight))
    values = low_back(matmul_high(rows, value_weight) + value_bias)
    context, proxy = attention_core(queries, keys, values, conv_weight, length)
    attended = low_back(matmul_high(low(context), output_weight) + output_bias)
    first_norm = layer_norm(rows + attended, norm_gain, norm_bias)
    up_rows = low_back(matmul_high(low(first_norm), up_weight) + up_bias)
    down_rows = low_back(matmul_high(low(gelu_exact(up_rows)), down_weight) + down_bias)
    return (layer_norm(first_norm + down_rows, final_gain, final_bias), proxy)

def reference(tokens, lengths, query_weight, key_weight, value_weight, query_bias, value_bias, conv_weight, output_weight, output_bias, norm_gain, norm_bias, up_weight, up_bias, down_weight, down_bias, final_gain, final_bias, cotangent):
    params = tuple((weight.astype(jnp.float32) for weight in (query_weight, key_weight, value_weight, query_bias, value_bias, conv_weight, output_weight, output_bias, norm_gain, norm_bias, up_weight, up_bias, down_weight, down_bias, final_gain, final_bias)))
    rows_all = tokens.astype(jnp.float32).reshape(SEQS, LEN, D)
    grads_all = cotangent.astype(jnp.float32).reshape(SEQS, LEN, D)

    def one_sequence(carry, item):
        rows, grad_rows, length = item

        def run(rows_in, params_in):
            return forward(rows_in, params_in, length)
        output_rows, backward, proxy_seq = jax.vjp(run, rows, params, has_aux=True)
        rows_grad, params_grad = backward(grad_rows)
        totals, proxy_total = carry
        totals = jax.tree.map(jnp.add, totals, params_grad)
        return ((totals, proxy_total + proxy_seq), (output_rows, rows_grad))
    start = (jax.tree.map(jnp.zeros_like, params), jnp.zeros((HEADS,), jnp.float32))
    (totals, proxy_total), (results, rows_grads) = lax.scan(one_sequence, start, (rows_all, grads_all, lengths))
    query_weight_grad, key_weight_grad, value_weight_grad, query_bias_grad, value_bias_grad, conv_weight_grad, output_weight_grad, output_bias_grad, norm_gain_grad, norm_bias_grad, up_weight_grad, up_bias_grad, down_weight_grad, down_bias_grad, final_gain_grad, final_bias_grad = totals
    return (results.reshape(TOKENS, D), rows_grads.reshape(TOKENS, D), query_weight_grad, key_weight_grad, value_weight_grad, query_bias_grad, value_bias_grad, conv_weight_grad, output_weight_grad, output_bias_grad, norm_gain_grad, norm_bias_grad, up_weight_grad, up_bias_grad, down_weight_grad, down_bias_grad, final_gain_grad, final_bias_grad, proxy_total / SEQS)
```

```python
import jax
import jax.numpy as jnp
from jax import lax
from jax.sharding import PartitionSpec as P

MARKS = 64
NEWTON = 6


EPSILON = 1e-05
MASKED_SCORE = 1000000000.0


def batch_mapped(form, left, right):
    return jnp.einsum(
        form, left, right, precision=lax.Precision.HIGHEST, preferred_element_type=jnp.float32
    )


def matmul(left, right):
    return jnp.dot(left, right, preferred_element_type=jnp.float32)


def matmul_left_t(left, right):
    return lax.dot_general(
        left, right, (((0,), (0,)), ((), ())), preferred_element_type=jnp.float32
    )


def matmul_right_t(left, right):
    return lax.dot_general(
        left, right, (((1,), (1,)), ((), ())), preferred_element_type=jnp.float32
    )


def softmax_final_axis(scores):
    top = jnp.max(scores, axis=-1, keepdims=True)
    powers = jnp.exp(scores - top)
    return powers / jnp.sum(powers, axis=-1, keepdims=True)


def newton_inverse(kernel):
    marks = kernel.shape[-1]
    identity = jnp.eye(marks, dtype=jnp.float32)
    column_max = jnp.max(jnp.sum(kernel, axis=-2), axis=-1)
    pseudo_inverse = jnp.swapaxes(kernel, -1, -2) / column_max[:, None, None]
    for sweep in range(NEWTON):
        product = batch_mapped("hmn,hnp->hmp", kernel, pseudo_inverse)
        inner = 7.0 * identity - product
        inner = 15.0 * identity - batch_mapped("hmn,hnp->hmp", product, inner)
        inner = 13.0 * identity - batch_mapped("hmn,hnp->hmp", product, inner)
        pseudo_inverse = 0.25 * batch_mapped("hmn,hnp->hmp", pseudo_inverse, inner)
    return pseudo_inverse


def attention_core(queries, keys, values, conv_weight, length):
    seq_len = queries.shape[0]
    heads = conv_weight.shape[0]
    width = conv_weight.shape[1]
    head_dim = queries.shape[1] // heads
    scale = head_dim ** (-0.25)
    marks = MARKS
    position = jnp.arange(seq_len, dtype=jnp.int32)
    valid_mask = (position < length).astype(jnp.float32)
    marker = jnp.arange(marks, dtype=jnp.int32)
    lower = marker * length // marks
    upper = (marker + 1) * length // marks
    inside = jnp.logical_and(
        position[None, :] >= lower[:, None], position[None, :] < upper[:, None]
    )
    counts = (upper - lower).astype(jnp.float32)
    segment_averager = inside.astype(jnp.float32) / counts[:, None]
    query_per_head = (queries * scale).reshape(seq_len, heads, head_dim)
    key_per_head = (keys * scale).reshape(seq_len, heads, head_dim)
    value_per_head = (values * valid_mask[:, None]).reshape(seq_len, heads, head_dim)
    query_landmarks = batch_mapped("vi,iqj->qvj", segment_averager, query_per_head)
    key_landmarks = batch_mapped("vi,iqj->qvj", segment_averager, key_per_head)
    first_kernel = softmax_final_axis(batch_mapped("bsz,scz->sbc", query_per_head, key_landmarks))
    second_kernel = softmax_final_axis(batch_mapped("pus,pos->puo", query_landmarks, key_landmarks))
    third_score_matrix = (
        batch_mapped("ncf,xnf->ncx", query_landmarks, key_per_head)
        + (valid_mask - 1.0) * MASKED_SCORE
    )
    third_kernel = softmax_final_axis(third_score_matrix)
    landmark_value_rows = batch_mapped("iob,bia->ioa", third_kernel, value_per_head)
    pseudo_inverse = newton_inverse(second_kernel)
    mixed_output = batch_mapped("xkc,xcl->xkl", pseudo_inverse, landmark_value_rows)
    nystrom_attention = batch_mapped("bqj,bjg->qbg", first_kernel, mixed_output)
    half = (width - 1) // 2
    padded = jnp.pad(value_per_head, ((half, half), (0, 0), (0, 0)))
    convolved = jnp.zeros_like(value_per_head)
    for offset in range(width):
        convolved = (
            convolved + conv_weight[:, offset][None, :, None] * padded[offset : offset + seq_len]
        )
    context = ((nystrom_attention + convolved) * valid_mask[:, None, None]).reshape(
        seq_len, heads * head_dim
    )
    proxy = (
        jnp.sqrt(jnp.sum(second_kernel * second_kernel, axis=(1, 2)))
        * jnp.sqrt(jnp.sum(pseudo_inverse * pseudo_inverse, axis=(1, 2)))
        / marks
    )
    return (context, proxy)


def layer_norm(rows, gain, shift):
    centered = rows - jnp.mean(rows, axis=-1, keepdims=True)
    variance = jnp.mean(centered * centered, axis=-1, keepdims=True)
    return centered * lax.rsqrt(variance + EPSILON) * gain + shift


def gelu_exact(values):
    return 0.5 * values * (1.0 + jax.scipy.special.erf(values * 0.5**0.5))


def column_sums(rows):
    return jnp.sum(rows.astype(jnp.float32), axis=0)


def pad_lanes(block):
    return jnp.pad(block, ((0, 0), (0, 128 - block.shape[1])))


def on_device(
    tokens,
    lengths,
    query_weight,
    key_weight,
    value_weight,
    query_bias,
    value_bias,
    conv_weight,
    output_weight,
    output_bias,
    norm_gain,
    norm_bias,
    up_weight,
    up_bias,
    down_weight,
    down_bias,
    final_gain,
    final_bias,
    cotangent,
):
    seq_count = lengths.shape[0]
    seq_len = tokens.shape[0] // seq_count
    width = tokens.shape[1]
    devices = lax.axis_size(("wide", "narrow"))
    shaped = (seq_count, seq_len, width)
    axes = ("wide", "narrow")
    units = query_bias.shape[0]
    ratio = up_bias.shape[0] // units
    hidden = up_weight.shape[1]
    small_one = pad_lanes(
        jnp.stack([query_bias, value_bias, output_bias, norm_gain, norm_bias], axis=1)
    )
    packed_one = jnp.concatenate(
        [query_weight, key_weight, value_weight, output_weight, small_one], axis=1
    )
    up_mixed = up_weight.reshape(units, width, ratio).swapaxes(1, 2).reshape(units, hidden)
    small_two = pad_lanes(
        jnp.concatenate(
            [
                up_bias.reshape(units, ratio),
                jnp.stack([down_bias, final_gain, final_bias], axis=1),
            ],
            axis=1,
        )
    )
    packed_two = jnp.concatenate(
        [up_mixed, down_weight.reshape(units, hidden), small_two], axis=1
    )
    full_one = lax.all_gather(packed_one, axes, axis=0, tiled=True)
    full_two = lax.all_gather(packed_two, axes, axis=0, tiled=True)
    query_full = full_one[:, :width]
    key_full = full_one[:, width : 2 * width]
    value_full = full_one[:, 2 * width : 3 * width]
    output_full = full_one[:, 3 * width : 4 * width]
    query_add, value_add, output_add, gain_one, shift_one = (
        full_one[:, 4 * width + n] for n in range(5)
    )
    up_full = full_two[:, :hidden]
    down_full = (
        full_two[:, hidden : 2 * hidden]
        .reshape(width, ratio, width)
        .swapaxes(0, 1)
        .reshape(hidden, width)
    )
    tail = full_two[:, 2 * hidden :]
    up_add = tail[:, :ratio].T.reshape(hidden)
    down_add, gain_two, shift_two = (tail[:, ratio + n] for n in range(3))
    queries = matmul(tokens, query_full) + query_add.astype(jnp.float32)
    keys = matmul(tokens, key_full)
    values = matmul(tokens, value_full) + value_add.astype(jnp.float32)
    conv_float = conv_weight.astype(jnp.float32)

    def core_batch(query_in, key_in, value_in, conv_in):
        return jax.vmap(attention_core, in_axes=(0, 0, 0, None, 0))(
            query_in, key_in, value_in, conv_in, lengths
        )

    context, core_back, proxies = jax.vjp(
        core_batch,
        queries.reshape(shaped),
        keys.reshape(shaped),
        values.reshape(shaped),
        conv_float,
        has_aux=True,
    )
    context_low = context.reshape(tokens.shape).astype(jnp.bfloat16)
    first_sum = (
        tokens.astype(jnp.float32)
        + matmul(context_low, output_full)
        + output_add.astype(jnp.float32)
    )
    first_norm, norm_back = jax.vjp(
        layer_norm, first_sum, gain_one.astype(jnp.float32), shift_one.astype(jnp.float32)
    )
    hidden_low = first_norm.astype(jnp.bfloat16)
    up_rows = matmul(hidden_low, up_full) + up_add.astype(jnp.float32)
    activated, gelu_back = jax.vjp(gelu_exact, up_rows)
    activated_low = activated.astype(jnp.bfloat16)
    second_sum = first_norm + matmul(activated_low, down_full) + down_add.astype(jnp.float32)
    result, final_back = jax.vjp(
        layer_norm, second_sum, gain_two.astype(jnp.float32), shift_two.astype(jnp.float32)
    )
    up_back = up_full
    down_back = down_full
    second_grad, final_gain_grad, final_bias_grad = final_back(cotangent.astype(jnp.float32))
    down_in = second_grad.astype(jnp.bfloat16)
    down_weight_grad = matmul_left_t(activated_low, down_in)
    down_bias_grad = column_sums(down_in)
    (up_grad,) = gelu_back(matmul_right_t(down_in, down_back))
    up_in = up_grad.astype(jnp.bfloat16)
    up_weight_grad = matmul_left_t(hidden_low, up_in)
    up_bias_grad = column_sums(up_in)
    hidden_grad = second_grad + matmul_right_t(up_in, up_back)
    down_mixed = (
        down_weight_grad.reshape(ratio, width, width).swapaxes(0, 1).reshape(width, hidden)
    )
    feed_owned = lax.psum_scatter(
        jnp.concatenate([up_weight_grad, down_mixed], axis=1).astype(jnp.bfloat16),
        axes,
        scatter_dimension=0,
        tiled=True,
    ).astype(jnp.float32)
    up_owned = feed_owned[:, :hidden].reshape(units, ratio, width).swapaxes(1, 2)
    down_owned = feed_owned[:, hidden:].reshape(units * ratio, width)
    query_back, key_back, value_back, output_back = query_full, key_full, value_full, output_full
    first_grad, norm_gain_grad, norm_bias_grad = norm_back(hidden_grad)
    attend_in = first_grad.astype(jnp.bfloat16)
    output_weight_grad = matmul_left_t(context_low, attend_in)
    output_bias_grad = column_sums(attend_in)
    context_grad = matmul_right_t(attend_in, output_back).reshape(shaped)
    query_grad, key_grad, value_grad, conv_grad = core_back(context_grad)
    query_in = query_grad.reshape(tokens.shape).astype(jnp.bfloat16)
    key_in = key_grad.reshape(tokens.shape).astype(jnp.bfloat16)
    value_in = value_grad.reshape(tokens.shape).astype(jnp.bfloat16)
    query_weight_grad = matmul_left_t(tokens, query_in)
    key_weight_grad = matmul_left_t(tokens, key_in)
    value_weight_grad = matmul_left_t(tokens, value_in)
    query_bias_grad = column_sums(query_in)
    value_bias_grad = column_sums(value_in)
    tokens_grad = (
        first_grad
        + matmul_right_t(query_in, query_back)
        + matmul_right_t(key_in, key_back)
        + matmul_right_t(value_in, value_back)
    )
    attention_owned = lax.psum_scatter(
        jnp.concatenate(
            [query_weight_grad, key_weight_grad, value_weight_grad, output_weight_grad], axis=1
        ).astype(jnp.bfloat16),
        axes,
        scatter_dimension=0,
        tiled=True,
    ).astype(jnp.float32)
    columns = jnp.stack(
        [
            query_bias_grad,
            value_bias_grad,
            output_bias_grad,
            norm_gain_grad,
            norm_bias_grad,
            down_bias_grad,
            final_gain_grad,
            final_bias_grad,
        ]
    )
    columns, up_bias_total, proxy_total, conv_total = lax.psum(
        (columns, up_bias_grad.reshape(ratio, width), jnp.sum(proxies, axis=0), conv_grad), axes
    )
    own = lax.axis_index(axes) * units
    columns = lax.dynamic_slice_in_dim(columns, own, units, axis=1)
    up_bias_owned = lax.dynamic_slice_in_dim(up_bias_total, own, units, axis=1).T.reshape(-1)
    proxy = proxy_total / (seq_count * devices)
    return (
        result,
        tokens_grad,
        attention_owned[:, :width],
        attention_owned[:, width : 2 * width],
        attention_owned[:, 2 * width : 3 * width],
        columns[0],
        columns[1],
        conv_total,
        attention_owned[:, 3 * width :],
        columns[2],
        columns[3],
        columns[4],
        up_owned.reshape(units, hidden),
        up_bias_owned,
        down_owned,
        columns[5],
        columns[6],
        columns[7],
        proxy,
    )


def solution(mesh):
    return jax.shard_map(
        on_device,
        mesh=mesh,
        in_specs=(
            P(("wide", "narrow"), None),
            P(("wide", "narrow")),
            P(("wide", "narrow"), None),
            P(("wide", "narrow"), None),
            P(("wide", "narrow"), None),
            P(("wide", "narrow")),
            P(("wide", "narrow")),
            P(),
            P(("wide", "narrow"), None),
            P(("wide", "narrow")),
            P(("wide", "narrow")),
            P(("wide", "narrow")),
            P(("wide", "narrow"), None),
            P(("wide", "narrow")),
            P(("wide", "narrow"), None),
            P(("wide", "narrow")),
            P(("wide", "narrow")),
            P(("wide", "narrow")),
            P(("wide", "narrow"), None),
        ),
        out_specs=(
            P(("wide", "narrow"), None),
            P(("wide", "narrow"), None),
            P(("wide", "narrow"), None),
            P(("wide", "narrow"), None),
            P(("wide", "narrow"), None),
            P(("wide", "narrow")),
            P(("wide", "narrow")),
            P(),
            P(("wide", "narrow"), None),
            P(("wide", "narrow")),
            P(("wide", "narrow")),
            P(("wide", "narrow")),
            P(("wide", "narrow"), None),
            P(("wide", "narrow")),
            P(("wide", "narrow"), None),
            P(("wide", "narrow")),
            P(("wide", "narrow")),
            P(("wide", "narrow")),
            P(),
        ),
        check_vma=False,
    )
```

```python
import jax
import jax.numpy as jnp
from jax import lax
from jax.experimental import pallas as pl
from jax.experimental.pallas import tpu as pltpu
from jax.sharding import PartitionSpec as P

MARKS = 64
NEWTON = 6


EPSILON = 1e-05
MASKED_SCORE = 1000000000.0


def batch_mapped(form, left, right):
    return jnp.einsum(
        form, left, right, precision=lax.Precision.HIGHEST, preferred_element_type=jnp.float32
    )


def matmul(left, right):
    return jnp.dot(left, right, preferred_element_type=jnp.float32)


def matmul_left_t(left, right):
    return lax.dot_general(
        left, right, (((0,), (0,)), ((), ())), preferred_element_type=jnp.float32
    )


def matmul_right_t(left, right):
    return lax.dot_general(
        left, right, (((1,), (1,)), ((), ())), preferred_element_type=jnp.float32
    )


def softmax_final_axis(scores):
    top = jnp.max(scores, axis=-1, keepdims=True)
    powers = jnp.exp(scores - top)
    return powers / jnp.sum(powers, axis=-1, keepdims=True)


def newton_inverse(kernel):
    marks = kernel.shape[-1]
    identity = jnp.eye(marks, dtype=jnp.float32)
    column_max = jnp.max(jnp.sum(kernel, axis=-2), axis=-1)
    pseudo_inverse = jnp.swapaxes(kernel, -1, -2) / column_max[:, None, None]
    for sweep in range(NEWTON):
        product = batch_mapped("hmn,hnp->hmp", kernel, pseudo_inverse)
        inner = 7.0 * identity - product
        inner = 15.0 * identity - batch_mapped("hmn,hnp->hmp", product, inner)
        inner = 13.0 * identity - batch_mapped("hmn,hnp->hmp", product, inner)
        pseudo_inverse = 0.25 * batch_mapped("hmn,hnp->hmp", pseudo_inverse, inner)
    return pseudo_inverse


def attention_core(queries, keys, values, heads, length):
    seq_len = queries.shape[0]
    head_dim = queries.shape[1] // heads
    scale = head_dim ** (-0.25)
    marks = MARKS
    position = jnp.arange(seq_len, dtype=jnp.int32)
    valid_mask = (position < length).astype(jnp.float32)
    marker = jnp.arange(marks, dtype=jnp.int32)
    lower = marker * length // marks
    upper = (marker + 1) * length // marks
    inside = jnp.logical_and(
        position[None, :] >= lower[:, None], position[None, :] < upper[:, None]
    )
    counts = (upper - lower).astype(jnp.float32)
    segment_averager = inside.astype(jnp.float32) / counts[:, None]
    query_per_head = (queries * scale).reshape(seq_len, heads, head_dim)
    key_per_head = (keys * scale).reshape(seq_len, heads, head_dim)
    value_per_head = (values * valid_mask[:, None]).reshape(seq_len, heads, head_dim)
    query_landmarks = batch_mapped("vi,iqj->qvj", segment_averager, query_per_head)
    key_landmarks = batch_mapped("vi,iqj->qvj", segment_averager, key_per_head)
    first_kernel = softmax_final_axis(batch_mapped("bsz,scz->sbc", query_per_head, key_landmarks))
    second_kernel = softmax_final_axis(batch_mapped("pus,pos->puo", query_landmarks, key_landmarks))
    third_score_matrix = (
        batch_mapped("ncf,xnf->ncx", query_landmarks, key_per_head)
        + (valid_mask - 1.0) * MASKED_SCORE
    )
    third_kernel = softmax_final_axis(third_score_matrix)
    landmark_value_rows = batch_mapped("iob,bia->ioa", third_kernel, value_per_head)
    pseudo_inverse = newton_inverse(second_kernel)
    mixed_output = batch_mapped("xkc,xcl->xkl", pseudo_inverse, landmark_value_rows)
    nystrom_attention = batch_mapped("bqj,bjg->qbg", first_kernel, mixed_output)
    context = (nystrom_attention * valid_mask[:, None, None]).reshape(seq_len, heads * head_dim)
    proxy = (
        jnp.sqrt(jnp.sum(second_kernel * second_kernel, axis=(1, 2)))
        * jnp.sqrt(jnp.sum(pseudo_inverse * pseudo_inverse, axis=(1, 2)))
        / marks
    )
    return (context, proxy)


BLOCK = 128
WINDOW = 256
DEPTH = 64


def banded(taps):
    return pltpu.roll(
        jnp.broadcast_to(taps, (BLOCK, WINDOW)), 0, 1, stride=1, stride_axis=0
    )


def fill_window(window_ref, rows, half):
    span = rows.shape[0]
    window_ref[:half] = jnp.zeros((half, rows.shape[1]), window_ref.dtype)
    window_ref[half : half + span] = rows.astype(window_ref.dtype)
    rest = window_ref.shape[0] - half - span
    window_ref[half + span :] = jnp.zeros((rest, rows.shape[1]), window_ref.dtype)


def banded_apply(taps_ref, window_refs, out_ref):
    bands = jnp.concatenate([banded(taps_ref[0, 0:1]), banded(taps_ref[0, 1:2])], axis=0)
    bands = bands.astype(jnp.bfloat16)
    first = lax.broadcasted_iota(jnp.int32, (BLOCK, 2 * DEPTH), 1) < DEPTH
    for block in range(out_ref.shape[0] // BLOCK):
        both = sum(
            matmul(bands, ref[block * BLOCK : block * BLOCK + WINDOW]) for ref in window_refs
        )
        out_ref[block * BLOCK : (block + 1) * BLOCK] = jnp.where(
            first, both[:BLOCK], both[BLOCK:]
        )


def conv_kernel(half, taps_ref, rows_ref, out_ref, high_ref, low_ref):
    rows = rows_ref[...]
    high = rows.astype(jnp.bfloat16)
    fill_window(high_ref, high, half)
    fill_window(low_ref, rows - high.astype(jnp.float32), half)
    banded_apply(taps_ref, (high_ref, low_ref), out_ref)


def conv_back_kernel(half, taps_ref, rows_ref, grad_ref, out_ref, tap_grad_ref, rows_win, grad_win):
    fill_window(rows_win, rows_ref[...], half)
    fill_window(grad_win, grad_ref[...], half)
    banded_apply(taps_ref, (grad_win,), out_ref)
    first = lax.broadcasted_iota(jnp.int32, (BLOCK, 2 * DEPTH), 1) < DEPTH
    total = jnp.zeros((2 * BLOCK, WINDOW), jnp.float32)
    row = lax.broadcasted_iota(jnp.int32, (BLOCK, BLOCK), 0)
    column = lax.broadcasted_iota(jnp.int32, (BLOCK, BLOCK), 1)
    flip = (row + column == BLOCK - 1).astype(jnp.float32).astype(jnp.bfloat16)
    for block in range(out_ref.shape[0] // BLOCK):
        grad = matmul(
            flip, grad_ref[block * BLOCK : (block + 1) * BLOCK].astype(jnp.bfloat16)
        )
        both = jnp.concatenate(
            [jnp.where(first, grad, 0.0), jnp.where(first, 0.0, grad)], axis=0
        ).astype(jnp.bfloat16)
        total += matmul_right_t(both, rows_win[block * BLOCK : block * BLOCK + WINDOW])
    for head in range(2):
        turned = pltpu.roll(
            total[head * BLOCK : (head + 1) * BLOCK],
            0,
            1,
            stride=1,
            stride_axis=0,
        )
        tap_grad_ref[0, head : head + 1] = jnp.sum(turned, axis=0, keepdims=True)


def conv_specs(rows):
    pair = pl.BlockSpec((rows.shape[0], 2 * DEPTH), lambda p: (0, p))
    taps = pl.BlockSpec((1, 2, WINDOW), lambda p: (p, 0, 0))
    return pair, taps


def window_scratch(rows):
    return pltpu.VMEM((rows.shape[0] + WINDOW, 2 * DEPTH), jnp.bfloat16)


def pair_taps(weight):
    heads, count = weight.shape
    return jnp.pad(weight, ((0, 0), (0, WINDOW - count))).reshape(heads // 2, 2, WINDOW)


def conv_forward(rows, weight):
    pair, taps = conv_specs(rows)
    return pl.pallas_call(
        lambda *refs: conv_kernel((weight.shape[1] - 1) // 2, *refs),
        grid=(weight.shape[0] // 2,),
        in_specs=[taps, pair],
        out_specs=pair,
        out_shape=jax.ShapeDtypeStruct(rows.shape, jnp.float32),
        scratch_shapes=[window_scratch(rows)] * 2,
        name="conv_forward",
    )(pair_taps(weight), rows)


def conv_backward(rows, grad, weight):
    pair, taps = conv_specs(rows)
    heads, count = weight.shape
    rows_grad, tap_grad = pl.pallas_call(
        lambda *refs: conv_back_kernel((count - 1) // 2, *refs),
        grid=(heads // 2,),
        in_specs=[taps, pair, pair],
        out_specs=[pair, taps],
        out_shape=[
            jax.ShapeDtypeStruct(rows.shape, jnp.float32),
            jax.ShapeDtypeStruct((heads // 2, 2, WINDOW), jnp.float32),
        ],
        scratch_shapes=[window_scratch(rows)] * 2,
        name="conv_backward",
    )(pair_taps(weight[:, ::-1]), rows, grad)
    return rows_grad, tap_grad.reshape(heads, WINDOW)[:, BLOCK - 1 : BLOCK - 1 + count]


def layer_norm(rows, gain, shift):
    centered = rows - jnp.mean(rows, axis=-1, keepdims=True)
    variance = jnp.mean(centered * centered, axis=-1, keepdims=True)
    return centered * lax.rsqrt(variance + EPSILON) * gain + shift


def gelu_exact(values):
    return 0.5 * values * (1.0 + jax.scipy.special.erf(values * 0.5**0.5))


def column_sums(rows):
    return jnp.sum(rows.astype(jnp.float32), axis=0)


def pad_lanes(block):
    return jnp.pad(block, ((0, 0), (0, 128 - block.shape[1])))


def on_device(
    tokens,
    lengths,
    query_weight,
    key_weight,
    value_weight,
    query_bias,
    value_bias,
    conv_weight,
    output_weight,
    output_bias,
    norm_gain,
    norm_bias,
    up_weight,
    up_bias,
    down_weight,
    down_bias,
    final_gain,
    final_bias,
    cotangent,
):
    seq_count = lengths.shape[0]
    seq_len = tokens.shape[0] // seq_count
    width = tokens.shape[1]
    devices = lax.axis_size(("wide", "narrow"))
    shaped = (seq_count, seq_len, width)
    axes = ("wide", "narrow")
    units = query_bias.shape[0]
    ratio = up_bias.shape[0] // units
    hidden = up_weight.shape[1]
    small_one = pad_lanes(
        jnp.stack([query_bias, value_bias, output_bias, norm_gain, norm_bias], axis=1)
    )
    packed_one = jnp.concatenate(
        [query_weight, key_weight, value_weight, output_weight, small_one], axis=1
    )
    up_mixed = up_weight.reshape(units, width, ratio).swapaxes(1, 2).reshape(units, hidden)
    small_two = pad_lanes(
        jnp.concatenate(
            [
                up_bias.reshape(units, ratio),
                jnp.stack([down_bias, final_gain, final_bias], axis=1),
            ],
            axis=1,
        )
    )
    packed_two = jnp.concatenate(
        [up_mixed, down_weight.reshape(units, hidden), small_two], axis=1
    )
    full_one = lax.all_gather(packed_one, axes, axis=0, tiled=True)
    full_two = lax.all_gather(packed_two, axes, axis=0, tiled=True)
    query_full = full_one[:, :width]
    key_full = full_one[:, width : 2 * width]
    value_full = full_one[:, 2 * width : 3 * width]
    output_full = full_one[:, 3 * width : 4 * width]
    query_add, value_add, output_add, gain_one, shift_one = (
        full_one[:, 4 * width + n] for n in range(5)
    )
    up_full = full_two[:, :hidden]
    down_full = (
        full_two[:, hidden : 2 * hidden]
        .reshape(width, ratio, width)
        .swapaxes(0, 1)
        .reshape(hidden, width)
    )
    tail = full_two[:, 2 * hidden :]
    up_add = tail[:, :ratio].T.reshape(hidden)
    down_add, gain_two, shift_two = (tail[:, ratio + n] for n in range(3))
    queries = matmul(tokens, query_full) + query_add.astype(jnp.float32)
    keys = matmul(tokens, key_full)
    values = matmul(tokens, value_full) + value_add.astype(jnp.float32)
    conv_float = conv_weight.astype(jnp.float32)

    heads = conv_weight.shape[0]
    live = (jnp.arange(seq_len, dtype=jnp.int32) < lengths[0]).astype(jnp.float32)[:, None]

    def core_batch(query_in, key_in, value_in):
        return jax.vmap(attention_core, in_axes=(0, 0, 0, None, 0))(
            query_in, key_in, value_in, heads, lengths
        )

    masked = values * live
    convolved = conv_forward(masked, conv_float)
    context, core_back, proxies = jax.vjp(
        core_batch,
        queries.reshape(shaped),
        keys.reshape(shaped),
        values.reshape(shaped),
        has_aux=True,
    )
    context_low = (context.reshape(tokens.shape) + convolved * live).astype(jnp.bfloat16)
    first_sum = (
        tokens.astype(jnp.float32)
        + matmul(context_low, output_full)
        + output_add.astype(jnp.float32)
    )
    first_norm, norm_back = jax.vjp(
        layer_norm, first_sum, gain_one.astype(jnp.float32), shift_one.astype(jnp.float32)
    )
    hidden_low = first_norm.astype(jnp.bfloat16)
    up_rows = matmul(hidden_low, up_full) + up_add.astype(jnp.float32)
    activated, gelu_back = jax.vjp(gelu_exact, up_rows)
    activated_low = activated.astype(jnp.bfloat16)
    second_sum = first_norm + matmul(activated_low, down_full) + down_add.astype(jnp.float32)
    result, final_back = jax.vjp(
        layer_norm, second_sum, gain_two.astype(jnp.float32), shift_two.astype(jnp.float32)
    )
    up_back = up_full
    down_back = down_full
    second_grad, final_gain_grad, final_bias_grad = final_back(cotangent.astype(jnp.float32))
    down_in = second_grad.astype(jnp.bfloat16)
    down_weight_grad = matmul_left_t(activated_low, down_in)
    down_bias_grad = column_sums(down_in)
    (up_grad,) = gelu_back(matmul_right_t(down_in, down_back))
    up_in = up_grad.astype(jnp.bfloat16)
    up_weight_grad = matmul_left_t(hidden_low, up_in)
    up_bias_grad = column_sums(up_in)
    hidden_grad = second_grad + matmul_right_t(up_in, up_back)
    down_mixed = (
        down_weight_grad.reshape(ratio, width, width).swapaxes(0, 1).reshape(width, hidden)
    )
    feed_packed = jnp.concatenate([up_weight_grad, down_mixed], axis=1).astype(jnp.bfloat16)
    feed_packed, hidden_grad = lax.optimization_barrier((feed_packed, hidden_grad))
    feed_owned = lax.psum_scatter(
        feed_packed,
        axes,
        scatter_dimension=0,
        tiled=True,
    ).astype(jnp.float32)
    up_owned = feed_owned[:, :hidden].reshape(units, ratio, width).swapaxes(1, 2)
    down_owned = feed_owned[:, hidden:].reshape(units * ratio, width)
    query_back, key_back, value_back, output_back = query_full, key_full, value_full, output_full
    first_grad, norm_gain_grad, norm_bias_grad = norm_back(hidden_grad)
    attend_in = first_grad.astype(jnp.bfloat16)
    output_weight_grad = matmul_left_t(context_low, attend_in)
    output_bias_grad = column_sums(attend_in)
    context_grad = matmul_right_t(attend_in, output_back)
    query_grad, key_grad, value_grad = core_back(context_grad.reshape(shaped))
    masked_grad, conv_grad = conv_backward(masked, context_grad * live, conv_float)
    value_grad = value_grad.reshape(tokens.shape) + masked_grad * live
    query_in = query_grad.reshape(tokens.shape).astype(jnp.bfloat16)
    key_in = key_grad.reshape(tokens.shape).astype(jnp.bfloat16)
    value_in = value_grad.reshape(tokens.shape).astype(jnp.bfloat16)
    query_weight_grad = matmul_left_t(tokens, query_in)
    key_weight_grad = matmul_left_t(tokens, key_in)
    value_weight_grad = matmul_left_t(tokens, value_in)
    query_bias_grad = column_sums(query_in)
    value_bias_grad = column_sums(value_in)
    tokens_grad = (
        first_grad
        + matmul_right_t(query_in, query_back)
        + matmul_right_t(key_in, key_back)
        + matmul_right_t(value_in, value_back)
    )
    attention_owned = lax.psum_scatter(
        jnp.concatenate(
            [query_weight_grad, key_weight_grad, value_weight_grad, output_weight_grad], axis=1
        ).astype(jnp.bfloat16),
        axes,
        scatter_dimension=0,
        tiled=True,
    ).astype(jnp.float32)
    columns = jnp.stack(
        [
            query_bias_grad,
            value_bias_grad,
            output_bias_grad,
            norm_gain_grad,
            norm_bias_grad,
            down_bias_grad,
            final_gain_grad,
            final_bias_grad,
        ]
    )
    columns, up_bias_total, proxy_total, conv_total = lax.psum(
        (columns, up_bias_grad.reshape(ratio, width), jnp.sum(proxies, axis=0), conv_grad), axes
    )
    own = lax.axis_index(axes) * units
    columns = lax.dynamic_slice_in_dim(columns, own, units, axis=1)
    up_bias_owned = lax.dynamic_slice_in_dim(up_bias_total, own, units, axis=1).T.reshape(-1)
    proxy = proxy_total / (seq_count * devices)
    return (
        result,
        tokens_grad,
        attention_owned[:, :width],
        attention_owned[:, width : 2 * width],
        attention_owned[:, 2 * width : 3 * width],
        columns[0],
        columns[1],
        conv_total,
        attention_owned[:, 3 * width :],
        columns[2],
        columns[3],
        columns[4],
        up_owned.reshape(units, hidden),
        up_bias_owned,
        down_owned,
        columns[5],
        columns[6],
        columns[7],
        proxy,
    )


def solution(mesh):
    return jax.shard_map(
        on_device,
        mesh=mesh,
        in_specs=(
            P(("wide", "narrow"), None),
            P(("wide", "narrow")),
            P(("wide", "narrow"), None),
            P(("wide", "narrow"), None),
            P(("wide", "narrow"), None),
            P(("wide", "narrow")),
            P(("wide", "narrow")),
            P(),
            P(("wide", "narrow"), None),
            P(("wide", "narrow")),
            P(("wide", "narrow")),
            P(("wide", "narrow")),
            P(("wide", "narrow"), None),
            P(("wide", "narrow")),
            P(("wide", "narrow"), None),
            P(("wide", "narrow")),
            P(("wide", "narrow")),
            P(("wide", "narrow")),
            P(("wide", "narrow"), None),
        ),
        out_specs=(
            P(("wide", "narrow"), None),
            P(("wide", "narrow"), None),
            P(("wide", "narrow"), None),
            P(("wide", "narrow"), None),
            P(("wide", "narrow"), None),
            P(("wide", "narrow")),
            P(("wide", "narrow")),
            P(),
            P(("wide", "narrow"), None),
            P(("wide", "narrow")),
            P(("wide", "narrow")),
            P(("wide", "narrow")),
            P(("wide", "narrow"), None),
            P(("wide", "narrow")),
            P(("wide", "narrow"), None),
            P(("wide", "narrow")),
            P(("wide", "narrow")),
            P(("wide", "narrow")),
            P(),
        ),
        check_vma=False,
    )
```
